32 devices in a mesh: seq: 16 (over z, y, x), head: 2 (over core).
Axes of the slice: x: 2, y: 2, z: 4, core: 2. Of those that a mesh axis runs over, the one named last changes fastest.
Arguments:
- hidden: bfloat16 [8192, 8192], P('seq', 'head'), may hold values from -6 to 6
- key_weight: bfloat16 [8192, 1024], P('head'), may hold values from -0.0625 to 0.0625
- value_weight: bfloat16 [8192, 1024], P('head'), may hold values from -0.0625 to 0.0625
- key_bias: float32 [1024], P('head'), may hold values from -5 to 5
- value_bias: float32 [1024], P('head'), may hold values from -5 to 5
- request_tokens: int32 [16], replicated, may hold values from 1 to 1024, 8192 in all
- request_context: int32 [16], replicated, may hold values from 0 to 4095
- page_owner: int32 [1024], replicated, may hold values from 0 to 15, as said below
- page_slot: int32 [1024], replicated, may hold values from 0 to 78
- key_cache: bfloat16 [1264, 8, 1024], P('seq', None, 'head'), may hold values from -1 to 1
- value_cache: bfloat16 [1264, 8, 1024], P('seq', None, 'head'), may hold values from -1 to 1
- stored_key_scales: bfloat16 [1264, 8], P('seq', 'head'), may hold values from 0.5 to 8
- value_scales: bfloat16 [1264, 8], P('seq', 'head'), may hold values from 0.5 to 8
Outputs:
- new_key_cache: bfloat16 [1264, 8, 1024], P('seq', None, 'head')
- new_value_cache: bfloat16 [1264, 8, 1024], P('seq', None, 'head')
- new_key_scales: bfloat16 [1264, 8], P('seq', 'head')
- new_value_scales: bfloat16 [1264, 8], P('seq', 'head')
The draws below stay inside these ranges and needn't reach their ends.
Inputs may be any that keep to these rules, and one draw needn't show every extreme that they name: No two pages name the same (page_owner, page_slot) pair. Each index of seq owns at most 79 pages of the block, and one owns exactly 79 in every draw. The 64 pages of one index of seq (pages i * 64 to (i + 1) * 64 - 1) go at most 5 to one owner, and some index sends exactly 5 to one owner in every draw.
All inputs are finite; a program needn't handle non-finite values.
Results may differ from the reference program's by a relative error of at most 0.0065.
Values may be sent and summed in bfloat16 or wider, within the bound.
A program may use at most 128 MiB of HBM per device.

```python
import math
import jax
import jax.numpy as jnp
import numpy as np

D = 8192
KVH = 8
HD = 128
PAGE = 8
REQS = 16
TOKENS = 8192
PAGES_DEV = 64
PAGES = 1024
SLOTS_DEV = 79
SLOTS = 1264
N_SEQ = 16


def page_table(key):
    base_key = jax.random.fold_in(key, 7)
    first, second, third, fourth = jax.random.split(base_key, 4)
    count = N_SEQ
    per_dev = PAGES_DEV
    window = SLOTS_DEV - PAGES_DEV
    order = jax.random.permutation(first, count)
    shift_zero = jax.random.randint(second, (), 0, count)
    hot_index = jax.random.randint(third, (), 0, count)
    page_ids = jnp.arange(count * per_dev).astype(jnp.int32)
    senders = page_ids // per_dev
    within = page_ids % per_dev
    normal_index = (senders + shift_zero - within) % count
    anchor = (hot_index - shift_zero) % count
    distance = (senders - anchor) % count
    moved = (within == 0) & (distance >= 1) & (distance <= window)
    index = jnp.where(moved, hot_index, normal_index)
    owner = order[index].astype(jnp.int32)
    earlier = (owner[:, None] == owner[None, :]) & (page_ids[None, :] < page_ids[:, None])
    rank = jnp.sum(earlier.astype(jnp.int32), axis=1)
    offsets = jax.random.randint(fourth, (count,), 0, SLOTS_DEV)
    slot = ((offsets[owner] + rank) % SLOTS_DEV).astype(jnp.int32)
    return (owner, slot)


def draw_page_owner(key, part):
    return page_table(key)[0]


def draw_page_slot(key, part):
    return page_table(key)[1]


def set_ends(result, key, low, high):
    place = [jax.random.randint(jax.random.fold_in(key, axis), (), 0, length) for axis, length in enumerate(result.shape)]
    main_axis = result.shape.index(max(result.shape))
    next_to = place[:main_axis] + [(place[main_axis] + 1) % result.shape[main_axis]] + place[main_axis + 1:]
    return result.at[tuple(place)].set(low).at[tuple(next_to)].set(high)


def block_scale(rng, dims, pieces, least, high):
    level = 1.0
    for dim, parts in pieces:
        draws = jax.random.uniform(jax.random.fold_in(jax.random.fold_in(rng, 6), dim), (parts,), jnp.float32, least / len(pieces), high / len(pieces))
        level = level * jnp.repeat(jnp.exp(draws), dims[dim] // parts).reshape((-1,) + (1,) * (len(dims) - 1 - dim))
    return level


def profile(amount, total, reach, slope):
    weights = [(1 << 20) // math.isqrt(rank ** slope) + 1 for rank in range(2, amount + 1)]
    surplus, given = total - reach - (amount - 1), [1] * (amount - 1)
    while surplus > 0:
        movable = [i for i in range(amount - 1) if given[i] < reach]
        pool, left = sum([weights[i] for i in movable]), surplus
        for i in movable:
            addition = min(reach - given[i], max(1, left * weights[i] // pool), surplus)
            given[i] = given[i] + addition
            surplus = surplus - addition
    return np.array([reach] + given)


def uneven_parts(stream_key, amount, total, most, lean):
    if amount == 2:
        one = jax.random.randint(stream_key, (), max(1, total - most), min(most, total - 1) + 1)
        return jnp.stack([one, total - one])
    sizes = jnp.asarray(profile(amount, total, most, lean), jnp.int32)
    couples = (amount - 1) // 2
    giver, receiver = sizes[1:1 + 2 * couples:2], sizes[2:2 + 2 * couples:2]
    room = jnp.minimum(giver - 1, most - receiver)
    shifted = jax.random.randint(jax.random.fold_in(stream_key, 1), (couples,), 0, 1 << 20) % (room + 1)
    sizes = sizes.at[1:1 + 2 * couples:2].set(giver - shifted).at[2:2 + 2 * couples:2].set(receiver + shifted)
    return sizes[jax.random.permutation(jax.random.fold_in(stream_key, 2), amount)]


def noise(own_key, dims, spread, most, pieces=(), held_as=jnp.bfloat16):
    values = spread * jax.random.normal(own_key, dims, jnp.float32)
    if pieces:
        values = values * block_scale(own_key, dims, pieces, -0.22, 0.18)
    return jnp.clip(values, -most, most).astype(held_as)


def setup_inputs(seed: int = 0) -> dict:
    seeds = jax.random.split(jax.random.key(seed), 14)
    return {
        "hidden": noise(seeds[0], (TOKENS, D), 1.0, 6.0, ((0, 16), (1, 2))),
        "key_weight": noise(seeds[1], (D, KVH * HD), D ** -0.5, 0.0625, ((0, 2),)),
        "value_weight": noise(seeds[2], (D, KVH * HD), D ** -0.5, 0.0625, ((0, 2),)),
        "key_bias": noise(seeds[3], (KVH * HD,), 1.0, 5.0, ((0, 2),), jnp.float32),
        "value_bias": noise(seeds[4], (KVH * HD,), 1.0, 5.0, ((0, 2),), jnp.float32),
        "request_tokens": uneven_parts(seeds[5], REQS, TOKENS, TOKENS // 8, 2).astype(jnp.int32),
        "request_context": set_ends(jax.random.randint(seeds[6], (REQS,), 0, 4096), jax.random.fold_in(seeds[6], 1), 0, 4095).astype(jnp.int32),
        "page_owner": draw_page_owner(jax.random.fold_in(seeds[13], 71), 0),
        "page_slot": draw_page_slot(jax.random.fold_in(seeds[13], 71), 0),
        "key_cache": jnp.clip(jax.random.uniform(seeds[9], (SLOTS, PAGE, KVH * HD), jnp.float32, -1.0, 1.0) * block_scale(seeds[9], (SLOTS, PAGE, KVH * HD), ((0, 16), (2, 2)), -0.4, 0.0), -1.0, 1.0).astype(jnp.bfloat16),
        "value_cache": jnp.clip(jax.random.uniform(seeds[10], (SLOTS, PAGE, KVH * HD), jnp.float32, -1.0, 1.0) * block_scale(seeds[10], (SLOTS, PAGE, KVH * HD), ((0, 16), (2, 2)), -0.4, 0.0), -1.0, 1.0).astype(jnp.bfloat16),
        "stored_key_scales": jnp.clip(jnp.exp(math.log(8.0) - 2.7725887 * jax.random.uniform(seeds[11], (SLOTS, KVH), jnp.float32) ** block_scale(seeds[11], (SLOTS, KVH), ((0, 16), (1, 2)), -0.2, 0.2)), 0.5, 8.0).astype(jnp.bfloat16),
        "value_scales": jnp.clip(jnp.exp(math.log(8.0) - 2.7725887 * jax.random.uniform(seeds[12], (SLOTS, KVH), jnp.float32) ** block_scale(seeds[12], (SLOTS, KVH), ((0, 16), (1, 2)), -0.2, 0.2)), 0.5, 8.0).astype(jnp.bfloat16),
    }


rope_base = 1000000.0
eps = 1e-6


def positions_of(request_tokens, request_context, token_ids):
    ends = jnp.cumsum(request_tokens).astype(jnp.int32)
    starts = ends - request_tokens
    inside = (token_ids[:, None] >= starts[None, :]) & (token_ids[:, None] < ends[None, :])
    offset = jnp.sum(jnp.where(inside, (request_context - starts)[None, :], 0), axis=1).astype(jnp.int32)
    return offset + token_ids


def rotate(values, positions, head_dim):
    half = head_dim // 2
    freqs = jnp.exp(-jnp.log(jnp.float32(rope_base)) * (2.0 * jnp.arange(half).astype(jnp.float32) / head_dim))
    angle = positions.astype(jnp.float32)[:, None] * freqs[None, :]
    cosine = jnp.cos(angle)[:, None, :]
    sine = jnp.sin(angle)[:, None, :]
    first = values[..., :half]
    second = values[..., half:]
    return jnp.concatenate([first * cosine - second * sine, second * cosine + first * sine], axis=-1)


def normalize(pages):
    largest = jnp.max(jnp.abs(pages.astype(jnp.float32)), axis=(1, 3))
    scale = (largest + eps).astype(jnp.bfloat16)
    codes = (pages.astype(jnp.float32) / scale.astype(jnp.float32)[:, None, :, None]).astype(jnp.bfloat16)
    return codes, scale


def reference(hidden, key_weight, value_weight, key_bias, value_bias, request_tokens, request_context, page_owner, page_slot, key_cache, value_cache, stored_key_scales, value_scales):
    token_ids = jnp.arange(TOKENS).astype(jnp.int32)
    positions = positions_of(request_tokens, request_context, token_ids)
    key_raw = jnp.dot(hidden, key_weight, preferred_element_type=jnp.float32) + key_bias
    value_raw = jnp.dot(hidden, value_weight, preferred_element_type=jnp.float32) + value_bias
    keys = rotate(key_raw.reshape(TOKENS, KVH, HD), positions, HD).astype(jnp.bfloat16)
    values = value_raw.reshape(TOKENS, KVH, HD).astype(jnp.bfloat16)
    key_codes, key_page_scale = normalize(keys.reshape(PAGES, PAGE, KVH, HD))
    value_codes, value_scale = normalize(values.reshape(PAGES, PAGE, KVH, HD))
    target = (page_owner * SLOTS_DEV + page_slot).astype(jnp.int32)
    new_key_cache = key_cache.at[target].set(key_codes.reshape(PAGES, PAGE, KVH * HD))
    new_value_cache = value_cache.at[target].set(value_codes.reshape(PAGES, PAGE, KVH * HD))
    new_key_scales = stored_key_scales.at[target].set(key_page_scale)
    new_value_scales = value_scales.at[target].set(value_scale)
    return new_key_cache, new_value_cache, new_key_scales, new_value_scales
```

```python
import functools
import math

import jax
import jax.numpy as jnp
from jax import lax
from jax.experimental import pallas as pl
from jax.experimental.pallas import tpu as pltpu
from jax.sharding import PartitionSpec as P

rope_base = 1000000.0
eps = 1e-06
KS = 4
MESH = pl.DeviceIdType.MESH


def body(
    n, cap, heads, hd, page, slots,
    own_in, slot_in, kb_in, vb_in, rt_in, rc_in,
    h_hbm, kw_hbm, vw_hbm, kc_hbm, vc_hbm,
    cache_v, spread_v,
    h_v, w_v, p_v, u_v, part_s, part_r, own_v, bias_v, send_v, recv_v, scale_v,
    cos_v, sin_v, sr_v,
    own_ref, slot_ref, kb_ref, vb_ref, rt_ref, rc_ref,
    h_sem, w0_sem, w_sem, c_sem, ps_sem, pr_sem, s_sem, r_sem, i_sem,
):
    toks, depth = h_v.shape
    kd = depth // KS
    chunks = 2 * heads
    half_cols = heads * hd
    f32, b16 = jnp.float32, jnp.bfloat16

    me = lax.axis_index("seq")
    side = lax.axis_index("head")
    other = 1 - side

    barrier = pltpu.get_barrier_semaphore()
    pl.semaphore_signal(barrier, inc=1, device_id={"head": other}, device_id_type=MESH)

    def greet(k, carry):
        pl.semaphore_signal(
            barrier, inc=1, device_id={"seq": lax.rem(me + k, n)}, device_id_type=MESH
        )
        return carry

    lax.fori_loop(1, n, greet, 0)

    def w_copies(c, rows, sem):
        src = vw_hbm if c < heads else kw_hbm
        copies = []
        for o, owner in enumerate((other, side)):
            col = pl.multiple_of(owner * half_cols + (c % heads) * hd, hd)
            copies.append(
                pltpu.make_async_copy(
                    src.at[rows, pl.ds(col, hd)], w_v.at[c, rows, pl.ds(o * hd, hd)], sem
                )
            )
        return copies

    def h_copy(s):
        part = pl.ds(s * kd, kd)
        return pltpu.make_async_copy(h_hbm.at[:, part], h_v.at[:, part], h_sem.at[s])

    pairs = (
        (own_in, own_ref), (slot_in, slot_ref), (kb_in, kb_ref),
        (vb_in, vb_ref), (rt_in, rt_ref), (rc_in, rc_ref),
    )
    small = [
        pltpu.make_async_copy(src, dst, i_sem.at[i]) for i, (src, dst) in enumerate(pairs)
    ]
    small[0].start()
    for s in range(KS):
        h_copy(s).start()
        for copy in w_copies(0, pl.ds(s * kd, kd), w0_sem.at[s]):
            copy.start()
    for copy in small[1:]:
        copy.start()
    for copy in w_copies(1, pl.ds(0, depth), w_sem.at[1]):
        copy.start()
    for copy in small:
        copy.wait()

    for c in range(chunks):
        src = vb_ref if c < heads else kb_ref
        bias_v[c] = src[:, pl.ds((c % heads) * hd, hd)]
    total_pages = own_ref.shape[1]
    here = total_pages // n
    owner = own_ref[...]
    gid = lax.broadcasted_iota(jnp.int32, (1, total_pages), 1)
    within = gid % here
    match = lax.broadcasted_iota(jnp.int32, (n, total_pages), 0) == owner
    count = jnp.where(match, 1.0, 0.0)
    shift = 1
    while shift < here:
        count = count + jnp.where(within >= shift, pltpu.roll(count, shift, 1), 0.0)
        shift *= 2
    rank = jnp.sum(jnp.where(match, count, 0.0), axis=0, keepdims=True) - 1.0
    place = ((owner - me + n) % n * cap).astype(f32) + rank
    place = pltpu.roll(
        jnp.broadcast_to(place, (8, total_pages)), (total_pages - me * here) % total_pages, 1
    )[:, :here]
    expand = (
        lax.broadcasted_iota(jnp.int32, (here, toks), 0)
        == lax.broadcasted_iota(jnp.int32, (here, toks), 1) // page
    )
    place = jnp.dot(
        place.astype(b16),
        jnp.where(expand, 1.0, 0.0).astype(b16),
        preferred_element_type=f32,
    )[:1]
    token = lax.broadcasted_iota(jnp.int32, (1, toks), 1)
    dk = place * page + (token % page).astype(f32)
    rows = lax.broadcasted_iota(jnp.int32, p_v.shape, 0).astype(f32)
    p_v[...] = jnp.where(rows == dk, 1.0, 0.0).astype(b16)

    def unpack_table():
        slot = jnp.where(owner == me, slot_ref[...], -1)
        lane = (((me - gid // here + n) % n) * cap).astype(f32) + rank + 1.0
        want = lax.broadcasted_iota(jnp.int32, (u_v.shape[0], 1), 0)
        src = jnp.sum(jnp.where(want // page == slot, lane, 0.0), axis=1, keepdims=True) - 1.0
        sr_v[...] = jnp.where(src >= 0.0, src * page + (want % page).astype(f32), -1.0)
        lanes = lax.broadcasted_iota(jnp.int32, u_v.shape, 1).astype(f32)
        u_v[...] = jnp.where(lanes == sr_v[...], 1.0, 0.0).astype(b16)

    def rope_table():
        half = hd // 2
        lane = (lax.broadcasted_iota(jnp.int32, (1, hd), 1) % half).astype(f32)
        freq = jnp.exp(-jnp.float32(math.log(rope_base)) * (2.0 * lane / hd))
        token_ids = me * toks + lax.broadcasted_iota(jnp.int32, cos_v.shape, 0)
        offset = jnp.zeros_like(token_ids)
        start = jnp.int32(0)
        for r in range(rt_ref.shape[0]):
            offset = jnp.where(token_ids >= start, rc_ref[r] - start, offset)
            start = start + rt_ref[r]
        angle = (offset + token_ids).astype(f32) * freq
        cos_v[...] = jnp.cos(angle)
        sine = jnp.sin(angle)
        front = lax.broadcasted_iota(jnp.int32, cos_v.shape, 1) < half
        sin_v[...] = jnp.where(front, -sine, sine)

    cos_v[...] = jnp.ones_like(cos_v)
    sin_v[...] = jnp.zeros_like(sin_v)
    scale_v[...] = jnp.zeros_like(scale_v)

    def swap(c):
        return pltpu.make_async_remote_copy(
            src_ref=part_s.at[c],
            dst_ref=part_r.at[c],
            send_sem=ps_sem.at[c],
            recv_sem=pr_sem.at[c],
            device_id={"head": other},
            device_id_type=MESH,
        )

    def post(c):
        swap(c).wait()
        x = own_v[c % 2] + part_r[c] + bias_v[c]
        x = x * cos_v[...] + pltpu.roll(x, hd // 2, 1) * sin_v[...]
        placed = jnp.dot(p_v[...], x.astype(b16), preferred_element_type=f32)
        placed = placed.reshape(n * cap, page, hd).astype(b16)
        send_v[c] = placed
        recv_v[c, :cap] = placed[:cap]

        def send(k, carry):
            pltpu.make_async_remote_copy(
                src_ref=send_v.at[c, pl.ds(k * cap, cap)],
                dst_ref=recv_v.at[c, pl.ds(k * cap, cap)],
                send_sem=s_sem.at[c],
                recv_sem=r_sem.at[c],
                device_id={"seq": lax.rem(me + k, n)},
                device_id_type=MESH,
            ).start()
            return carry

        lax.fori_loop(1, n, send, 0)

    def first(s, carry):
        part = pl.ds(pl.multiple_of(s * kd, kd), kd)
        h_part = h_v.at[:, part]
        w_part = w_v.at[0, part]
        pltpu.make_async_copy(h_part, h_part, h_sem.at[s]).wait()
        pltpu.make_async_copy(w_part, w_part, w0_sem.at[s]).wait()
        got = jnp.dot(h_part[...], w_part[...], preferred_element_type=f32)

        @pl.when(s == 0)
        def _():
            part_s[0] = got[:, :hd]
            own_v[0] = got[:, hd:]

        @pl.when(s > 0)
        def _():
            part_s[0] = part_s[0] + got[:, :hd]
            own_v[0] = own_v[0] + got[:, hd:]

        return carry

    lax.fori_loop(0, KS, first, 0)
    for copy in w_copies(2, pl.ds(0, depth), w_sem.at[2]):
        copy.start()
    pl.semaphore_wait(barrier, n)
    swap(0).start()

    def produce(c, carry):
        for i in range(3, chunks):
            @pl.when(c == i - 2)
            def _():
                for copy in w_copies(i, pl.ds(0, depth), w_sem.at[i]):
                    copy.start()

        @pl.when(c == chunks - 2)
        def _():
            pltpu.make_async_copy(vc_hbm, cache_v.at[0], c_sem.at[0]).start()
            pltpu.make_async_copy(kc_hbm, cache_v.at[1], c_sem.at[1]).start()

        w_all = w_v.at[c]
        pltpu.make_async_copy(w_all, w_all, w_sem.at[c]).wait()
        got = jnp.dot(h_v[...], w_all[...], preferred_element_type=f32)
        part_s[c] = got[:, :hd]
        own_v[c % 2] = got[:, hd:]
        swap(c).start()
        post(c - 1)

        @pl.when(c == heads)
        def _():
            rope_table()

        return carry

    lax.fori_loop(1, chunks, produce, 0)
    post(chunks - 1)

    unpack_table()
    head_lane = lax.broadcasted_iota(jnp.int32, (1, 1, hd), 2)
    written = (sr_v[...] >= 0.0)[: slots * page]
    for i in range(2):
        pltpu.make_async_copy(cache_v.at[i], cache_v.at[i], c_sem.at[i]).wait()

    def consume(c, carry):
        rest = recv_v.at[c, pl.ds(cap, (n - 1) * cap)]
        pltpu.make_async_copy(rest, rest, r_sem.at[c]).wait()
        x = recv_v[c].astype(f32)
        largest = jnp.max(jnp.max(jnp.abs(x), axis=1, keepdims=True), axis=2, keepdims=True)
        scale = (largest + eps).astype(b16).astype(f32)
        scales = scale_v[...] + jnp.where(head_lane == c, scale, 0.0)
        scale_v[...] = scales
        codes = (x / scale).reshape(n * cap * page, hd)
        flat = jnp.broadcast_to(scales, (n * cap, page, hd)).reshape(n * cap * page, hd)
        both = jnp.concatenate([codes, flat], axis=1).astype(b16)
        placed = jnp.dot(u_v[...], both, preferred_element_type=f32)
        spread_v[...] = placed[:, hd:]
        lanes = pl.ds(pl.multiple_of((c % heads) * hd, hd), hd)
        old = cache_v[c // heads, :, :, lanes].astype(f32).reshape(slots * page, hd)
        new = jnp.where(written, placed[: slots * page, :hd], old)
        cache_v[c // heads, :, :, lanes] = new.reshape(slots, page, hd).astype(b16)
        return carry

    lax.fori_loop(0, chunks, consume, 0)

    for c in range(chunks):
        out = send_v.at[c, pl.ds(cap, (n - 1) * cap)]
        pltpu.make_async_copy(out, out, s_sem.at[c]).wait()


def hand_on(
    heads, page, slots,
    cache_v, spread_ref, oks_ref, ovs_ref,
    kc_out, vc_out, ks_out, vs_out,
    ks_v, vs_v, o_sem,
):
    f32 = jnp.float32
    copies = [
        pltpu.make_async_copy(cache_v.at[0], vc_out, o_sem.at[0]),
        pltpu.make_async_copy(cache_v.at[1], kc_out, o_sem.at[1]),
        pltpu.make_async_copy(vs_v, vs_out, o_sem.at[2]),
        pltpu.make_async_copy(ks_v, ks_out, o_sem.at[3]),
    ]
    for copy in copies[:2]:
        copy.start()
    hd = spread_ref.shape[1]
    spread = spread_ref[...][: slots * page].reshape(slots, page, hd)[:, 0, :]
    spread = jnp.concatenate([spread, jnp.zeros((128 - slots % 128, hd), f32)], axis=0)
    spread = jnp.transpose(spread)[:, :slots]
    vs_v[...] = jnp.where(
        spread[:heads] > 0.0, spread[:heads], ovs_ref[...].astype(f32)
    ).astype(jnp.bfloat16)
    ks_v[...] = jnp.where(
        spread[heads:2 * heads] > 0.0, spread[heads:2 * heads], oks_ref[...].astype(f32)
    ).astype(jnp.bfloat16)
    for copy in copies[2:]:
        copy.start()
    for copy in copies:
        copy.wait()


def shards(
    hidden,
    key_weight,
    value_weight,
    key_bias,
    value_bias,
    request_tokens,
    request_context,
    page_owner,
    page_slot,
    key_cache,
    value_cache,
    stored_key_scales,
    value_scales,
):
    toks, depth = hidden.shape
    slots, page, cols = key_cache.shape
    heads = stored_key_scales.shape[1]
    hd = cols // heads
    pages_here = toks // page
    n = lax.axis_size("seq")
    cap = (pages_here + n - 1) // n + 1
    rows = n * cap * page
    srows = (slots * page + 15) // 16 * 16
    chunks = 2 * heads
    vm = pl.BlockSpec(memory_space=pltpu.VMEM)
    hbm = pl.BlockSpec(memory_space=pl.ANY)
    f32, b16 = jnp.float32, jnp.bfloat16
    cache, spread = pl.pallas_call(
        functools.partial(body, n, cap, heads, hd, page, slots),
        out_shape=(
            pltpu.VMEM((2, slots, page, cols), b16),
            pltpu.VMEM((srows, hd), f32),
        ),
        in_specs=[hbm] * 11,
        out_specs=(vm, vm),
        scratch_shapes=[
            pltpu.VMEM((toks, depth), b16),
            pltpu.VMEM((chunks, depth, 2 * hd), b16),
            pltpu.VMEM((rows, toks), b16),
            pltpu.VMEM((srows, rows), b16),
            pltpu.VMEM((chunks, toks, hd), f32),
            pltpu.VMEM((chunks, toks, hd), f32),
            pltpu.VMEM((2, toks, hd), f32),
            pltpu.VMEM((chunks, 1, hd), f32),
            pltpu.VMEM((chunks, n * cap, page, hd), b16),
            pltpu.VMEM((chunks, n * cap, page, hd), b16),
            pltpu.VMEM((n * cap, 1, hd), f32),
            pltpu.VMEM((toks, hd), f32),
            pltpu.VMEM((toks, hd), f32),
            pltpu.VMEM((srows, 1), f32),
            pltpu.VMEM((1, page_owner.shape[0]), jnp.int32),
            pltpu.VMEM((1, page_owner.shape[0]), jnp.int32),
            pltpu.VMEM((1, cols), f32),
            pltpu.VMEM((1, cols), f32),
            pltpu.SMEM(request_tokens.shape, jnp.int32),
            pltpu.SMEM(request_tokens.shape, jnp.int32),
            pltpu.SemaphoreType.DMA((KS,)),
            pltpu.SemaphoreType.DMA((KS,)),
            pltpu.SemaphoreType.DMA((chunks,)),
            pltpu.SemaphoreType.DMA((2,)),
            pltpu.SemaphoreType.DMA((chunks,)),
            pltpu.SemaphoreType.DMA((chunks,)),
            pltpu.SemaphoreType.DMA((chunks,)),
            pltpu.SemaphoreType.DMA((chunks,)),
            pltpu.SemaphoreType.DMA((6,)),
        ],
        compiler_params=pltpu.CompilerParams(
            collective_id=0, has_side_effects=True, vmem_limit_bytes=48 * 1024 * 1024
        ),
    )(*[
        pltpu.with_memory_space_constraint(a, pltpu.HBM)
        for a in (
            page_owner.reshape(1, -1), page_slot.reshape(1, -1),
            key_bias.reshape(1, -1), value_bias.reshape(1, -1),
            request_tokens, request_context,
            hidden, key_weight, value_weight, key_cache, value_cache,
        )
    ])
    keys, values, key_scales, new_value_scales = pl.pallas_call(
        functools.partial(hand_on, heads, page, slots),
        out_shape=(
            jax.ShapeDtypeStruct(key_cache.shape, b16),
            jax.ShapeDtypeStruct(value_cache.shape, b16),
            jax.ShapeDtypeStruct((heads, slots), b16),
            jax.ShapeDtypeStruct((heads, slots), b16),
        ),
        in_specs=[vm] * 4,
        out_specs=(hbm,) * 4,
        scratch_shapes=[
            pltpu.VMEM((heads, slots), b16),
            pltpu.VMEM((heads, slots), b16),
            pltpu.SemaphoreType.DMA((4,)),
        ],
        compiler_params=pltpu.CompilerParams(vmem_limit_bytes=4 * 1024 * 1024),
    )(cache, spread, stored_key_scales.T, value_scales.T)
    return keys, values, key_scales.T, new_value_scales.T


def solution(mesh):
    placed = (
        P("seq", "head"),
        P("head", None),
        P("head", None),
        P("head"),
        P("head"),
        P(),
        P(),
        P(),
        P(),
        P("seq", None, "head"),
        P("seq", None, "head"),
        P("seq", "head"),
        P("seq", "head"),
    )
    return jax.shard_map(
        shards,
        mesh=mesh,
        in_specs=placed,
        out_specs=(
            P("seq", None, "head"),
            P("seq", None, "head"),
            P("seq", "head"),
            P("seq", "head"),
        ),
        check_vma=False,
    )
```

```python
import functools
import math

import jax
import jax.numpy as jnp
from jax import lax
from jax.experimental import pallas as pl
from jax.experimental.pallas import tpu as pltpu
from jax.sharding import PartitionSpec as P

rope_base = 1000000.0
eps = 1e-06
KS = 4
LATE = 3
MESH = pl.DeviceIdType.MESH


def groups_of(chunks):
    edges = [0, 1] + list(range(2, chunks - 2, 2)) + [chunks - 2, chunks - 1, chunks]
    return tuple(zip(edges, edges[1:]))


def coded(c, x, scales):
    count, page, hd = x.shape
    lane = lax.broadcasted_iota(jnp.int32, (1, 1, hd), 2)
    x = x.astype(jnp.float32)
    largest = jnp.max(jnp.max(jnp.abs(x), axis=1, keepdims=True), axis=2, keepdims=True)
    scale = (largest + eps).astype(jnp.bfloat16).astype(jnp.float32)
    codes = (x / scale).reshape(count * page, hd)
    return codes, scales + jnp.where(lane == c, scale, 0.0)


def body(
    n, cap, heads, hd, page, slots,
    own_in, slot_in, kb_in, vb_in, rt_in, rc_in,
    h_hbm, kw_hbm, vw_hbm, kc_hbm, vc_hbm,
    cache_v, last_v, u_v, sr_v, scale_v,
    h_v, w_v, p_v, part_s, part_r, own_v, bias_v, send_v, recv_v,
    cos_v, sin_v,
    own_ref, slot_ref, kb_ref, vb_ref, rt_ref, rc_ref,
    h_sem, w0_sem, w_sem, c_sem, ps_sem, pr_sem, s_sem, r_sem, i_sem,
):
    toks, depth = h_v.shape
    kd = depth // KS
    chunks = 2 * heads
    groups = groups_of(chunks)
    half_cols = heads * hd
    f32, b16 = jnp.float32, jnp.bfloat16

    me = lax.axis_index("seq")
    side = lax.axis_index("head")
    other = 1 - side

    def w_copy(c, o, rows, sem):
        src = vw_hbm if c < heads else kw_hbm
        owner = side if o else other
        col = pl.multiple_of(owner * half_cols + (c % heads) * hd, hd)
        return pltpu.make_async_copy(
            src.at[rows, pl.ds(col, hd)], w_v.at[c, rows, pl.ds(o * hd, hd)], sem
        )

    def w_start(c):
        for o in range(2):
            w_copy(c, o, pl.ds(0, depth), w_sem.at[c]).start()

    def h_copy(s):
        part = pl.ds(s * kd, kd)
        return pltpu.make_async_copy(h_hbm.at[:, part], h_v.at[:, part], h_sem.at[s])

    pairs = (
        (own_in, own_ref), (slot_in, slot_ref), (kb_in, kb_ref),
        (vb_in, vb_ref), (rt_in, rt_ref), (rc_in, rc_ref),
    )
    small = [
        pltpu.make_async_copy(src, dst, i_sem.at[i]) for i, (src, dst) in enumerate(pairs)
    ]
    small[0].start()
    for s in range(KS):
        h_copy(s).start()
        for o in range(2):
            w_copy(0, o, pl.ds(s * kd, kd), w0_sem.at[s]).start()

    barrier = pltpu.get_barrier_semaphore()
    pl.semaphore_signal(barrier, inc=1, device_id={"head": other}, device_id_type=MESH)

    def greet(k, carry):
        pl.semaphore_signal(
            barrier, inc=1, device_id={"seq": lax.rem(me + k, n)}, device_id_type=MESH
        )
        return carry

    lax.fori_loop(1, n, greet, 0)
    for copy in small[1:]:
        copy.start()
    w_start(1)

    def rope_table():
        half = hd // 2
        lane = (lax.broadcasted_iota(jnp.int32, (1, hd), 1) % half).astype(f32)
        freq = jnp.exp(-jnp.float32(math.log(rope_base)) * (2.0 * lane / hd))
        token_ids = me * toks + lax.broadcasted_iota(jnp.int32, cos_v.shape, 0)
        offset = jnp.zeros_like(token_ids)
        start = jnp.int32(0)
        for r in range(rt_ref.shape[0]):
            offset = jnp.where(token_ids >= start, rc_ref[r] - start, offset)
            start = start + rt_ref[r]
        angle = (offset + token_ids).astype(f32) * freq
        cos_v[...] = jnp.cos(angle)
        sine = jnp.sin(angle)
        front = lax.broadcasted_iota(jnp.int32, cos_v.shape, 1) < half
        sin_v[...] = jnp.where(front, -sine, sine)

    def swap(c):
        return pltpu.make_async_remote_copy(
            src_ref=part_s.at[c],
            dst_ref=part_r.at[c],
            send_sem=ps_sem.at[c],
            recv_sem=pr_sem.at[c],
            device_id={"head": other},
            device_id_type=MESH,
        )

    def launch(g, wanted):
        low, high = groups[g]
        part = pl.ds(low, high - low)

        def send(i, carry):
            there, spot = i // 4, (me + i) % 4
            dest = there * 4 + spot
            k = lax.rem(dest - me + n, n)
            steps = spot % 2 + spot // 2 + there % 2
            pick = dest != me
            if wanted is not None:
                pick = jnp.logical_and(pick, wanted(steps))

            @pl.when(pick)
            def _():
                pltpu.make_async_remote_copy(
                    src_ref=send_v.at[part, pl.ds(k * cap, cap)],
                    dst_ref=recv_v.at[part, pl.ds(k * cap, cap)],
                    send_sem=s_sem.at[g],
                    recv_sem=r_sem.at[g],
                    device_id={"seq": dest},
                    device_id_type=MESH,
                ).start()

            return carry

        lax.fori_loop(0, n, send, 0)

    def launches(g):
        late = len(groups) - LATE
        if g < late:
            launch(g, None)
            return
        launch(g, lambda steps: steps <= 1)
        if g == len(groups) - 1:
            for e in range(late, g):
                launch(e, lambda steps: steps > 1)
            launch(g, lambda steps: steps > 1)

    def post(c):
        swap(c).wait()
        x = own_v[c % 2] + part_r[c] + bias_v[c]
        x = x * cos_v[...] + pltpu.roll(x, hd // 2, 1) * sin_v[...]
        placed = jnp.dot(p_v[...], x.astype(b16), preferred_element_type=f32)
        placed = placed.reshape(n * cap, page, hd).astype(b16)
        send_v[c] = placed
        recv_v[c, :cap] = placed[:cap]
        for g, (low, high) in enumerate(groups):
            if isinstance(c, int):
                if high == c + 1:
                    launches(g)
            else:
                @pl.when(c == high - 1)
                def _():
                    launches(g)

    def first(s, carry):
        part = pl.ds(pl.multiple_of(s * kd, kd), kd)
        h_part = h_v.at[:, part]
        w_part = w_v.at[0, part]
        pltpu.make_async_copy(h_part, h_part, h_sem.at[s]).wait()
        pltpu.make_async_copy(w_part, w_part, w0_sem.at[s]).wait()
        got = jnp.dot(h_part[...], w_part[...], preferred_element_type=f32)

        @pl.when(s == 0)
        def _():
            part_s[0] = got[:, :hd]
            own_v[0] = got[:, hd:]

        @pl.when(s > 0)
        def _():
            part_s[0] = part_s[0] + got[:, :hd]
            own_v[0] = own_v[0] + got[:, hd:]

        return carry

    lax.fori_loop(0, KS, first, 0)
    w_start(2)
    pl.semaphore_wait(barrier, n)
    swap(0).start()
    small[0].wait()

    total_pages = own_ref.shape[1]
    here = total_pages // n
    owner = own_ref[...]
    gid = lax.broadcasted_iota(jnp.int32, (1, total_pages), 1)
    within = gid % here
    match = lax.broadcasted_iota(jnp.int32, (n, total_pages), 0) == owner
    count = jnp.where(match, 1.0, 0.0)
    shift = 1
    while shift < here:
        count = count + jnp.where(within >= shift, pltpu.roll(count, shift, 1), 0.0)
        shift *= 2
    rank = jnp.sum(jnp.where(match, count, 0.0), axis=0, keepdims=True) - 1.0
    place = ((owner - me + n) % n * cap).astype(f32) + rank
    place = pltpu.roll(
        jnp.broadcast_to(place, (8, total_pages)), (total_pages - me * here) % total_pages, 1
    )[:, :here]
    expand = (
        lax.broadcasted_iota(jnp.int32, (here, toks), 0)
        == lax.broadcasted_iota(jnp.int32, (here, toks), 1) // page
    )
    place = jnp.dot(
        place.astype(b16),
        jnp.where(expand, 1.0, 0.0).astype(b16),
        preferred_element_type=f32,
    )[:1]
    token = lax.broadcasted_iota(jnp.int32, (1, toks), 1)
    dk = place * page + (token % page).astype(f32)
    rows = lax.broadcasted_iota(jnp.int32, p_v.shape, 0).astype(f32)
    p_v[...] = jnp.where(rows == dk, 1.0, 0.0).astype(b16)

    cos_v[...] = jnp.ones_like(cos_v)
    sin_v[...] = jnp.zeros_like(sin_v)
    scale_v[...] = jnp.zeros_like(scale_v)

    def unpack_table():
        slot = jnp.where(owner == me, slot_ref[...], -1)
        lane = (((me - gid // here + n) % n) * cap).astype(f32) + rank + 1.0
        want = lax.broadcasted_iota(jnp.int32, (u_v.shape[0], 1), 0)
        src = jnp.sum(jnp.where(want // page == slot, lane, 0.0), axis=1, keepdims=True) - 1.0
        sr_v[...] = jnp.where(src >= 0.0, src * page + (want % page).astype(f32), -1.0)
        lanes = lax.broadcasted_iota(jnp.int32, u_v.shape, 1).astype(f32)
        u_v[...] = jnp.where(lanes == sr_v[...], 1.0, 0.0).astype(b16)

    for copy in small[1:]:
        copy.wait()
    for c in range(chunks):
        src = vb_ref if c < heads else kb_ref
        bias_v[c] = src[:, pl.ds((c % heads) * hd, hd)]
    post(0)

    def produce(c, carry):
        for i in range(3, chunks):
            @pl.when(c == i - 2)
            def _():
                w_start(i)

        @pl.when(c == chunks - 2)
        def _():
            pltpu.make_async_copy(vc_hbm, cache_v.at[0], c_sem.at[0]).start()
            pltpu.make_async_copy(kc_hbm, cache_v.at[1], c_sem.at[1]).start()

        w_all = w_v.at[c]
        pltpu.make_async_copy(w_all, w_all, w_sem.at[c]).wait()
        got = jnp.dot(h_v[...], w_all[...], preferred_element_type=f32)
        part_s[c] = got[:, :hd]
        own_v[c % 2] = got[:, hd:]
        swap(c).start()

        @pl.when(c > 1)
        def _():
            post(c - 1)

        @pl.when(c == heads)
        def _():
            rope_table()

        return carry

    lax.fori_loop(1, chunks, produce, 0)
    post(chunks - 1)

    unpack_table()
    written = (sr_v[...] >= 0.0)[: slots * page]
    for i in range(2):
        pltpu.make_async_copy(cache_v.at[i], cache_v.at[i], c_sem.at[i]).wait()

    def receive(c, carry):
        for g, (low, high) in enumerate(groups):
            @pl.when(c == low)
            def _():
                rest = recv_v.at[pl.ds(low, high - low), pl.ds(cap, (n - 1) * cap)]
                pltpu.make_async_copy(rest, rest, r_sem.at[g]).wait()

        @pl.when(c < chunks - 1)
        def _():
            codes, scale_v[...] = coded(c, recv_v[c], scale_v[...])
            placed = jnp.dot(u_v[...], codes.astype(b16), preferred_element_type=f32)
            lanes = pl.ds(pl.multiple_of((c % heads) * hd, hd), hd)
            old = cache_v[c // heads, :, :, lanes].astype(f32).reshape(slots * page, hd)
            new = jnp.where(written, placed[: slots * page], old)
            cache_v[c // heads, :, :, lanes] = new.reshape(slots, page, hd).astype(b16)

        return carry

    lax.fori_loop(0, chunks, receive, 0)
    last_v[...] = recv_v[chunks - 1]

    for g, (low, high) in enumerate(groups):
        out = send_v.at[pl.ds(low, high - low), pl.ds(cap, (n - 1) * cap)]
        pltpu.make_async_copy(out, out, s_sem.at[g]).wait()


def hand_on(
    heads, hd,
    held_v, last_v, u_v, sr_v, held_scale, oks_ref, ovs_ref,
    kc_out, vc_out, ks_out, vs_out,
    tail_v, ks_v, vs_v, o_sem,
):
    f32, b16 = jnp.float32, jnp.bfloat16
    slots, page = held_v.shape[1:3]
    cut = (heads - 1) * hd
    copies = [
        pltpu.make_async_copy(held_v.at[0], vc_out, o_sem.at[0]),
        pltpu.make_async_copy(
            held_v.at[1, :, :, pl.ds(0, cut)], kc_out.at[:, :, pl.ds(0, cut)], o_sem.at[1]
        ),
        pltpu.make_async_copy(tail_v, kc_out.at[:, :, pl.ds(cut, hd)], o_sem.at[2]),
        pltpu.make_async_copy(vs_v, vs_out, o_sem.at[3]),
        pltpu.make_async_copy(ks_v, ks_out, o_sem.at[4]),
    ]
    for copy in copies[:2]:
        copy.start()
    count = last_v.shape[0]
    codes, scales = coded(2 * heads - 1, last_v[...], held_scale[...])
    flat = jnp.broadcast_to(scales, (count, page, hd)).reshape(count * page, hd)
    both = jnp.concatenate([codes, flat], axis=1).astype(b16)
    placed = jnp.dot(u_v[...], both, preferred_element_type=f32)[: slots * page]
    written = (sr_v[...] >= 0.0)[: slots * page]
    old = held_v[1, :, :, cut:].astype(f32).reshape(slots * page, hd)
    new = jnp.where(written, placed[:, :hd], old)
    tail_v[...] = new.reshape(slots, page, hd).astype(b16)
    copies[2].start()
    spread = placed[:, hd:].reshape(slots, page, hd)[:, 0, :]
    spread = jnp.concatenate([spread, jnp.zeros((128 - slots % 128, hd), f32)], axis=0)
    spread = jnp.transpose(spread)[:, :slots]
    vs_v[...] = jnp.where(spread[:heads] > 0.0, spread[:heads], ovs_ref[...].astype(f32)).astype(b16)
    ks_v[...] = jnp.where(
        spread[heads:2 * heads] > 0.0, spread[heads:2 * heads], oks_ref[...].astype(f32)
    ).astype(b16)
    for copy in copies[3:]:
        copy.start()
    for copy in copies:
        copy.wait()


def shards(
    hidden,
    key_weight,
    value_weight,
    key_bias,
    value_bias,
    request_tokens,
    request_context,
    page_owner,
    page_slot,
    key_cache,
    value_cache,
    stored_key_scales,
    value_scales,
):
    toks, depth = hidden.shape
    slots, page, cols = key_cache.shape
    heads = stored_key_scales.shape[1]
    hd = cols // heads
    pages_here = toks // page
    n = lax.axis_size("seq")
    cap = (pages_here + n - 1) // n + 1
    rows = n * cap * page
    srows = (slots * page + 15) // 16 * 16
    chunks = 2 * heads
    groups = groups_of(chunks)
    vm = pl.BlockSpec(memory_space=pltpu.VMEM)
    hbm = pl.BlockSpec(memory_space=pl.ANY)
    f32, b16 = jnp.float32, jnp.bfloat16
    held = pl.pallas_call(
        functools.partial(body, n, cap, heads, hd, page, slots),
        out_shape=(
            pltpu.VMEM((2, slots, page, cols), b16),
            pltpu.VMEM((n * cap, page, hd), b16),
            pltpu.VMEM((srows, rows), b16),
            pltpu.VMEM((srows, 1), f32),
            pltpu.VMEM((n * cap, 1, hd), f32),
        ),
        in_specs=[hbm] * 11,
        out_specs=(vm,) * 5,
        scratch_shapes=[
            pltpu.VMEM((toks, depth), b16),
            pltpu.VMEM((chunks, depth, 2 * hd), b16),
            pltpu.VMEM((rows, toks), b16),
            pltpu.VMEM((chunks, toks, hd), f32),
            pltpu.VMEM((chunks, toks, hd), f32),
            pltpu.VMEM((2, toks, hd), f32),
            pltpu.VMEM((chunks, 1, hd), f32),
            pltpu.VMEM((chunks, n * cap, page, hd), b16),
            pltpu.VMEM((chunks, n * cap, page, hd), b16),
            pltpu.VMEM((toks, hd), f32),
            pltpu.VMEM((toks, hd), f32),
            pltpu.VMEM((1, page_owner.shape[0]), jnp.int32),
            pltpu.VMEM((1, page_owner.shape[0]), jnp.int32),
            pltpu.VMEM((1, cols), f32),
            pltpu.VMEM((1, cols), f32),
            pltpu.SMEM(request_tokens.shape, jnp.int32),
            pltpu.SMEM(request_tokens.shape, jnp.int32),
            pltpu.SemaphoreType.DMA((KS,)),
            pltpu.SemaphoreType.DMA((KS,)),
            pltpu.SemaphoreType.DMA((chunks,)),
            pltpu.SemaphoreType.DMA((2,)),
            pltpu.SemaphoreType.DMA((chunks,)),
            pltpu.SemaphoreType.DMA((chunks,)),
            pltpu.SemaphoreType.DMA((len(groups),)),
            pltpu.SemaphoreType.DMA((len(groups),)),
            pltpu.SemaphoreType.DMA((6,)),
        ],
        compiler_params=pltpu.CompilerParams(
            collective_id=0, has_side_effects=True, vmem_limit_bytes=48 * 1024 * 1024
        ),
    )(*[
        pltpu.with_memory_space_constraint(a, pltpu.HBM)
        for a in (
            page_owner.reshape(1, -1), page_slot.reshape(1, -1),
            key_bias.reshape(1, -1), value_bias.reshape(1, -1),
            request_tokens, request_context,
            hidden, key_weight, value_weight, key_cache, value_cache,
        )
    ])
    keys, values, key_scales, new_value_scales = pl.pallas_call(
        functools.partial(hand_on, heads, hd),
        out_shape=(
            jax.ShapeDtypeStruct(key_cache.shape, b16),
            jax.ShapeDtypeStruct(value_cache.shape, b16),
            jax.ShapeDtypeStruct((heads, slots), b16),
            jax.ShapeDtypeStruct((heads, slots), b16),
        ),
        in_specs=[vm] * 7,
        out_specs=(hbm,) * 4,
        scratch_shapes=[
            pltpu.VMEM((slots, page, hd), b16),
            pltpu.VMEM((heads, slots), b16),
            pltpu.VMEM((heads, slots), b16),
            pltpu.SemaphoreType.DMA((5,)),
        ],
        compiler_params=pltpu.CompilerParams(vmem_limit_bytes=8 * 1024 * 1024),
    )(*held, stored_key_scales.T, value_scales.T)
    return keys, values, key_scales.T, new_value_scales.T


def solution(mesh):
    placed = (
        P("seq", "head"),
        P("head", None),
        P("head", None),
        P("head"),
        P("head"),
        P(),
        P(),
        P(),
        P(),
        P("seq", None, "head"),
        P("seq", None, "head"),
        P("seq", "head"),
        P("seq", "head"),
    )
    return jax.shard_map(
        shards,
        mesh=mesh,
        in_specs=placed,
        out_specs=(
            P("seq", None, "head"),
            P("seq", None, "head"),
            P("seq", "head"),
            P("seq", "head"),
        ),
        check_vma=False,
    )
```

```python
import functools
import math

import jax
import jax.numpy as jnp
from jax import lax
from jax.experimental import pallas as pl
from jax.experimental.pallas import tpu as pltpu
from jax.sharding import PartitionSpec as P

rope_base = 1000000.0
eps = 1e-06
KS = 4
LATE = 3
MESH = pl.DeviceIdType.MESH


def groups_of(chunks):
    edges = [0, 1] + list(range(2, chunks - 2, 2)) + [chunks - 2, chunks - 1, chunks]
    return tuple(zip(edges, edges[1:]))


def coded(u_v, x, slots):
    count, page, hd = x.shape
    rows = x.astype(jnp.float32).reshape(count * page, hd).astype(jnp.bfloat16)
    placed = jnp.dot(u_v[...], rows, preferred_element_type=jnp.float32)
    placed = placed[: slots * page].reshape(slots, page, hd)
    largest = jnp.max(jnp.max(jnp.abs(placed), axis=1, keepdims=True), axis=2, keepdims=True)
    scale = (largest + eps).astype(jnp.bfloat16).astype(jnp.float32)
    return placed / scale, scale


def taken(sr_v, slots, page):
    row = sr_v[...][: slots * page].reshape(slots, page, 1)
    return jnp.max(row, axis=1, keepdims=True) >= 0.0


def body(
    n, cap, heads, hd, page, slots,
    own_in, slot_in, kb_in, vb_in, rt_in, rc_in,
    h_hbm, kw_hbm, vw_hbm, kc_hbm, vc_hbm,
    cache_v, last_v, u_v, sr_v, scale_v,
    h_v, w_v, p_v, part_s, part_r, own_v, bias_v, send_v, recv_v,
    cos_v, sin_v,
    own_ref, slot_ref, kb_ref, vb_ref, rt_ref, rc_ref,
    h_sem, w0_sem, w_sem, c_sem, ps_sem, pr_sem, s_sem, r_sem, i_sem,
):
    toks, depth = h_v.shape
    kd = depth // KS
    chunks = 2 * heads
    groups = groups_of(chunks)
    half_cols = heads * hd
    f32, b16 = jnp.float32, jnp.bfloat16

    me = lax.axis_index("seq")
    side = lax.axis_index("head")
    other = 1 - side

    def w_copy(c, o, rows, sem):
        src = vw_hbm if c < heads else kw_hbm
        owner = side if o else other
        col = pl.multiple_of(owner * half_cols + (c % heads) * hd, hd)
        return pltpu.make_async_copy(
            src.at[rows, pl.ds(col, hd)], w_v.at[c, rows, pl.ds(o * hd, hd)], sem
        )

    def w_start(c):
        for o in range(2):
            w_copy(c, o, pl.ds(0, depth), w_sem.at[c]).start()

    def h_copy(s):
        part = pl.ds(s * kd, kd)
        return pltpu.make_async_copy(h_hbm.at[:, part], h_v.at[:, part], h_sem.at[s])

    pairs = (
        (own_in, own_ref), (slot_in, slot_ref), (kb_in, kb_ref),
        (vb_in, vb_ref), (rt_in, rt_ref), (rc_in, rc_ref),
    )
    small = [
        pltpu.make_async_copy(src, dst, i_sem.at[i]) for i, (src, dst) in enumerate(pairs)
    ]
    small[0].start()
    for s in range(KS):
        h_copy(s).start()
        for o in range(2):
            w_copy(0, o, pl.ds(s * kd, kd), w0_sem.at[s]).start()

    barrier = pltpu.get_barrier_semaphore()
    pl.semaphore_signal(barrier, inc=1, device_id={"head": other}, device_id_type=MESH)

    def greet(k, carry):
        pl.semaphore_signal(
            barrier, inc=1, device_id={"seq": lax.rem(me + k, n)}, device_id_type=MESH
        )
        return carry

    lax.fori_loop(1, n, greet, 0)
    for copy in small[1:]:
        copy.start()
    w_start(1)

    def rope_table():
        half = hd // 2
        lane = (lax.broadcasted_iota(jnp.int32, (1, hd), 1) % half).astype(f32)
        freq = jnp.exp(-jnp.float32(math.log(rope_base)) * (2.0 * lane / hd))
        token_ids = me * toks + lax.broadcasted_iota(jnp.int32, cos_v.shape, 0)
        offset = jnp.zeros_like(token_ids)
        start = jnp.int32(0)
        for r in range(rt_ref.shape[0]):
            offset = jnp.where(token_ids >= start, rc_ref[r] - start, offset)
            start = start + rt_ref[r]
        angle = (offset + token_ids).astype(f32) * freq
        cos_v[...] = jnp.cos(angle)
        sine = jnp.sin(angle)
        front = lax.broadcasted_iota(jnp.int32, cos_v.shape, 1) < half
        sin_v[...] = jnp.where(front, -sine, sine)

    def swap(c):
        return pltpu.make_async_remote_copy(
            src_ref=part_s.at[c],
            dst_ref=part_r.at[c],
            send_sem=ps_sem.at[c],
            recv_sem=pr_sem.at[c],
            device_id={"head": other},
            device_id_type=MESH,
        )

    def launch(g, wanted):
        low, high = groups[g]
        part = pl.ds(low, high - low)

        def send(i, carry):
            there, spot = jnp.where(me < 8, 3 - i // 4, i // 4), (me + i) % 4
            dest = there * 4 + spot
            k = lax.rem(dest - me + n, n)
            steps = spot % 2 + spot // 2 + there % 2
            pick = dest != me
            if wanted is not None:
                pick = jnp.logical_and(pick, wanted(steps))

            @pl.when(pick)
            def _():
                pltpu.make_async_remote_copy(
                    src_ref=send_v.at[part, pl.ds(k * cap, cap)],
                    dst_ref=recv_v.at[part, pl.ds(k * cap, cap)],
                    send_sem=s_sem.at[g],
                    recv_sem=r_sem.at[g],
                    device_id={"seq": dest},
                    device_id_type=MESH,
                ).start()

            return carry

        lax.fori_loop(0, n, send, 0)

    def launches(g):
        late = len(groups) - LATE
        if g < late:
            launch(g, None)
            return
        launch(g, lambda steps: steps <= 1)
        if g == len(groups) - 1:
            launch(late, lambda steps: steps > 1)
            for e in range(late + 1, g + 1):
                launch(e, lambda steps: steps == 2)
            for e in range(late + 1, g + 1):
                launch(e, lambda steps: steps == 3)

    def post(c):
        swap(c).wait()
        x = own_v[c % 2] + part_r[c] + bias_v[c]
        x = x * cos_v[...] + pltpu.roll(x, hd // 2, 1) * sin_v[...]
        placed = jnp.dot(p_v[...], x.astype(b16), preferred_element_type=f32)
        placed = placed.reshape(n * cap, page, hd).astype(b16)
        send_v[c] = placed
        recv_v[c, :cap] = placed[:cap]
        for g, (low, high) in enumerate(groups):
            if isinstance(c, int):
                if high == c + 1:
                    launches(g)
            else:
                @pl.when(c == high - 1)
                def _():
                    launches(g)

    def first(s, carry):
        part = pl.ds(pl.multiple_of(s * kd, kd), kd)
        h_part = h_v.at[:, part]
        w_part = w_v.at[0, part]
        pltpu.make_async_copy(h_part, h_part, h_sem.at[s]).wait()
        pltpu.make_async_copy(w_part, w_part, w0_sem.at[s]).wait()
        got = jnp.dot(h_part[...], w_part[...], preferred_element_type=f32)

        @pl.when(s == 0)
        def _():
            part_s[0] = got[:, :hd]
            own_v[0] = got[:, hd:]

        @pl.when(s > 0)
        def _():
            part_s[0] = part_s[0] + got[:, :hd]
            own_v[0] = own_v[0] + got[:, hd:]

        return carry

    lax.fori_loop(0, KS, first, 0)
    w_start(2)
    pl.semaphore_wait(barrier, n)
    swap(0).start()
    small[0].wait()

    total_pages = own_ref.shape[1]
    here = total_pages // n
    owner = own_ref[...]
    gid = lax.broadcasted_iota(jnp.int32, (1, total_pages), 1)
    within = gid % here
    match = lax.broadcasted_iota(jnp.int32, (n, total_pages), 0) == owner
    count = jnp.where(match, 1.0, 0.0)
    shift = 1
    while shift < here:
        count = count + jnp.where(within >= shift, pltpu.roll(count, shift, 1), 0.0)
        shift *= 2
    rank = jnp.sum(jnp.where(match, count, 0.0), axis=0, keepdims=True) - 1.0
    place = ((owner - me + n) % n * cap).astype(f32) + rank
    place = pltpu.roll(
        jnp.broadcast_to(place, (8, total_pages)), (total_pages - me * here) % total_pages, 1
    )[:, :here]
    expand = (
        lax.broadcasted_iota(jnp.int32, (here, toks), 0)
        == lax.broadcasted_iota(jnp.int32, (here, toks), 1) // page
    )
    place = jnp.dot(
        place.astype(b16),
        jnp.where(expand, 1.0, 0.0).astype(b16),
        preferred_element_type=f32,
    )[:1]
    token = lax.broadcasted_iota(jnp.int32, (1, toks), 1)
    dk = place * page + (token % page).astype(f32)
    rows = lax.broadcasted_iota(jnp.int32, p_v.shape, 0).astype(f32)
    p_v[...] = jnp.where(rows == dk, 1.0, 0.0).astype(b16)

    cos_v[...] = jnp.ones_like(cos_v)
    sin_v[...] = jnp.zeros_like(sin_v)
    scale_v[...] = jnp.zeros_like(scale_v)

    def unpack_table():
        slot = jnp.where(owner == me, slot_ref[...], -1)
        lane = (((me - gid // here + n) % n) * cap).astype(f32) + rank + 1.0
        want = lax.broadcasted_iota(jnp.int32, (u_v.shape[0], 1), 0)
        src = jnp.sum(jnp.where(want // page == slot, lane, 0.0), axis=1, keepdims=True) - 1.0
        sr_v[...] = jnp.where(src >= 0.0, src * page + (want % page).astype(f32), -1.0)
        lanes = lax.broadcasted_iota(jnp.int32, u_v.shape, 1).astype(f32)
        u_v[...] = jnp.where(lanes == sr_v[...], 1.0, 0.0).astype(b16)

    for copy in small[1:]:
        copy.wait()
    for c in range(chunks):
        src = vb_ref if c < heads else kb_ref
        bias_v[c] = src[:, pl.ds((c % heads) * hd, hd)]
    post(0)

    def produce(c, carry):
        for i in range(3, chunks):
            @pl.when(c == i - 2)
            def _():
                w_start(i)

        @pl.when(c == chunks - 2)
        def _():
            pltpu.make_async_copy(vc_hbm, cache_v.at[0], c_sem.at[0]).start()
            pltpu.make_async_copy(kc_hbm, cache_v.at[1], c_sem.at[1]).start()

        w_all = w_v.at[c]
        pltpu.make_async_copy(w_all, w_all, w_sem.at[c]).wait()
        got = jnp.dot(h_v[...], w_all[...], preferred_element_type=f32)
        part_s[c] = got[:, :hd]
        own_v[c % 2] = got[:, hd:]
        swap(c).start()

        @pl.when(c > 1)
        def _():
            post(c - 1)

        @pl.when(c == heads)
        def _():
            rope_table()

        return carry

    lax.fori_loop(1, chunks, produce, 0)
    post(chunks - 1)

    unpack_table()
    written = taken(sr_v, slots, page)
    head_lane = lax.broadcasted_iota(jnp.int32, (1, 1, hd), 2)
    for i in range(2):
        pltpu.make_async_copy(cache_v.at[i], cache_v.at[i], c_sem.at[i]).wait()

    def receive(c, carry):
        for g, (low, high) in enumerate(groups):
            @pl.when(c == low)
            def _():
                rest = recv_v.at[pl.ds(low, high - low), pl.ds(cap, (n - 1) * cap)]
                pltpu.make_async_copy(rest, rest, r_sem.at[g]).wait()

        @pl.when(c < chunks - 1)
        def _():
            codes, scale = coded(u_v, recv_v[c], slots)
            scale_v[...] += jnp.where(written & (head_lane == c), scale, 0.0)
            lanes = pl.ds(pl.multiple_of((c % heads) * hd, hd), hd)
            old = cache_v[c // heads, :, :, lanes].astype(f32)
            cache_v[c // heads, :, :, lanes] = jnp.where(written, codes, old).astype(b16)

        return carry

    lax.fori_loop(0, chunks, receive, 0)
    last_v[...] = recv_v[chunks - 1]

    for g, (low, high) in enumerate(groups):
        out = send_v.at[pl.ds(low, high - low), pl.ds(cap, (n - 1) * cap)]
        pltpu.make_async_copy(out, out, s_sem.at[g]).wait()


def hand_on(
    heads, hd,
    held_v, last_v, u_v, sr_v, held_scale, oks_ref, ovs_ref,
    kc_out, vc_out, ks_out, vs_out,
    tail_v, ks_v, vs_v, o_sem,
):
    f32, b16 = jnp.float32, jnp.bfloat16
    slots, page = held_v.shape[1:3]
    cut = (heads - 1) * hd
    copies = [
        pltpu.make_async_copy(held_v.at[0], vc_out, o_sem.at[0]),
        pltpu.make_async_copy(
            held_v.at[1, :, :, pl.ds(0, cut)], kc_out.at[:, :, pl.ds(0, cut)], o_sem.at[1]
        ),
        pltpu.make_async_copy(tail_v, kc_out.at[:, :, pl.ds(cut, hd)], o_sem.at[2]),
        pltpu.make_async_copy(vs_v, vs_out, o_sem.at[3]),
        pltpu.make_async_copy(ks_v, ks_out, o_sem.at[4]),
    ]
    for copy in copies[:2]:
        copy.start()
    written = taken(sr_v, slots, page)
    head_lane = lax.broadcasted_iota(jnp.int32, (1, 1, hd), 2)
    codes, scale = coded(u_v, last_v[...], slots)
    old = held_v[1, :, :, cut:].astype(f32)
    tail_v[...] = jnp.where(written, codes, old).astype(b16)
    copies[2].start()
    scales = held_scale[...] + jnp.where(written & (head_lane == 2 * heads - 1), scale, 0.0)
    spread = scales[:, 0, :]
    spread = jnp.concatenate([spread, jnp.zeros((128 - slots % 128, hd), f32)], axis=0)
    spread = jnp.transpose(spread)[:, :slots]
    vs_v[...] = jnp.where(spread[:heads] > 0.0, spread[:heads], ovs_ref[...].astype(f32)).astype(b16)
    ks_v[...] = jnp.where(
        spread[heads:2 * heads] > 0.0, spread[heads:2 * heads], oks_ref[...].astype(f32)
    ).astype(b16)
    for copy in copies[3:]:
        copy.start()
    for copy in copies:
        copy.wait()


def shards(
    hidden,
    key_weight,
    value_weight,
    key_bias,
    value_bias,
    request_tokens,
    request_context,
    page_owner,
    page_slot,
    key_cache,
    value_cache,
    stored_key_scales,
    value_scales,
):
    toks, depth = hidden.shape
    slots, page, cols = key_cache.shape
    heads = stored_key_scales.shape[1]
    hd = cols // heads
    pages_here = toks // page
    n = lax.axis_size("seq")
    cap = (pages_here + n - 1) // n + 1
    rows = n * cap * page
    srows = (slots * page + 15) // 16 * 16
    chunks = 2 * heads
    groups = groups_of(chunks)
    vm = pl.BlockSpec(memory_space=pltpu.VMEM)
    hbm = pl.BlockSpec(memory_space=pl.ANY)
    f32, b16 = jnp.float32, jnp.bfloat16
    held = pl.pallas_call(
        functools.partial(body, n, cap, heads, hd, page, slots),
        out_shape=(
            pltpu.VMEM((2, slots, page, cols), b16),
            pltpu.VMEM((n * cap, page, hd), b16),
            pltpu.VMEM((srows, rows), b16),
            pltpu.VMEM((srows, 1), f32),
            pltpu.VMEM((slots, 1, hd), f32),
        ),
        in_specs=[hbm] * 11,
        out_specs=(vm,) * 5,
        scratch_shapes=[
            pltpu.VMEM((toks, depth), b16),
            pltpu.VMEM((chunks, depth, 2 * hd), b16),
            pltpu.VMEM((rows, toks), b16),
            pltpu.VMEM((chunks, toks, hd), f32),
            pltpu.VMEM((chunks, toks, hd), f32),
            pltpu.VMEM((2, toks, hd), f32),
            pltpu.VMEM((chunks, 1, hd), f32),
            pltpu.VMEM((chunks, n * cap, page, hd), b16),
            pltpu.VMEM((chunks, n * cap, page, hd), b16),
            pltpu.VMEM((toks, hd), f32),
            pltpu.VMEM((toks, hd), f32),
            pltpu.VMEM((1, page_owner.shape[0]), jnp.int32),
            pltpu.VMEM((1, page_owner.shape[0]), jnp.int32),
            pltpu.VMEM((1, cols), f32),
            pltpu.VMEM((1, cols), f32),
            pltpu.SMEM(request_tokens.shape, jnp.int32),
            pltpu.SMEM(request_tokens.shape, jnp.int32),
            pltpu.SemaphoreType.DMA((KS,)),
            pltpu.SemaphoreType.DMA((KS,)),
            pltpu.SemaphoreType.DMA((chunks,)),
            pltpu.SemaphoreType.DMA((2,)),
            pltpu.SemaphoreType.DMA((chunks,)),
            pltpu.SemaphoreType.DMA((chunks,)),
            pltpu.SemaphoreType.DMA((len(groups),)),
            pltpu.SemaphoreType.DMA((len(groups),)),
            pltpu.SemaphoreType.DMA((6,)),
        ],
        compiler_params=pltpu.CompilerParams(
            collective_id=0, has_side_effects=True, vmem_limit_bytes=48 * 1024 * 1024
        ),
    )(*[
        pltpu.with_memory_space_constraint(a, pltpu.HBM)
        for a in (
            page_owner.reshape(1, -1), page_slot.reshape(1, -1),
            key_bias.reshape(1, -1), value_bias.reshape(1, -1),
            request_tokens, request_context,
            hidden, key_weight, value_weight, key_cache, value_cache,
        )
    ])
    keys, values, key_scales, new_value_scales = pl.pallas_call(
        functools.partial(hand_on, heads, hd),
        out_shape=(
            jax.ShapeDtypeStruct(key_cache.shape, b16),
            jax.ShapeDtypeStruct(value_cache.shape, b16),
            jax.ShapeDtypeStruct((heads, slots), b16),
            jax.ShapeDtypeStruct((heads, slots), b16),
        ),
        in_specs=[vm] * 7,
        out_specs=(hbm,) * 4,
        scratch_shapes=[
            pltpu.VMEM((slots, page, hd), b16),
            pltpu.VMEM((heads, slots), b16),
            pltpu.VMEM((heads, slots), b16),
            pltpu.SemaphoreType.DMA((5,)),
        ],
        compiler_params=pltpu.CompilerParams(vmem_limit_bytes=8 * 1024 * 1024),
    )(*held, stored_key_scales.T, value_scales.T)
    return keys, values, key_scales.T, new_value_scales.T


def solution(mesh):
    placed = (
        P("seq", "head"),
        P("head", None),
        P("head", None),
        P("head"),
        P("head"),
        P(),
        P(),
        P(),
        P(),
        P("seq", None, "head"),
        P("seq", None, "head"),
        P("seq", "head"),
        P("seq", "head"),
    )
    return jax.shard_map(
        shards,
        mesh=mesh,
        in_specs=placed,
        out_specs=(
            P("seq", None, "head"),
            P("seq", None, "head"),
            P("seq", "head"),
            P("seq", "head"),
        ),
        check_vma=False,
    )
```
